16 devices in a mesh: rep: 2 (over y, z), dp: 8 (over x, core).
Axes of the slice: x: 4, y: 2, z: 1, core: 2. Of those that a mesh axis runs over, the one named last changes fastest.
The devices are a block of a 4x4x8 slice.
Arguments:
- x: bfloat16 [16, 2048, 896], P(('rep', 'dp')), parts along dimension 0
- dy: bfloat16 [16, 2048, 896], P(('rep', 'dp')), parts along dimension 0
- w_gate: bfloat16 [2, 896, 2304], P(None, 'dp')
- w_up: bfloat16 [2, 896, 2304], P(None, 'dp')
- w_down: bfloat16 [2, 2304, 896], P(None, 'dp')
Outputs:
- output 1: bfloat16 [16, 2048, 896], P(('rep', 'dp')), parts along dimension 0
- output 2: bfloat16 [4, 896, 2304], P('rep', 'dp'), parts along dimension 0
- output 3: bfloat16 [4, 896, 2304], P('rep', 'dp'), parts along dimension 0
- output 4: bfloat16 [4, 2304, 896], P('rep', 'dp'), parts along dimension 0
There are 2 independent parts. The reference program is written for one: setup_inputs(seed, part) draws one part's arguments, and reference() takes and returns one part's arrays. A program takes and returns all parts, laid end to end along the dimension named above; an argument that names none is the same for every part.
All inputs are finite; a program needn't handle non-finite values.
Results may differ from the reference program's by a relative error of at most 0.018.
Values are sent between devices in bfloat16 or wider.
A program may use at most 768 MiB of HBM per device.

```python
import jax
import jax.numpy as jnp
from jax import lax

SEQUENCES = 8
TOKENS = 2048
D = 896
FF = 2304
LAYERS = 2
NAMES = ("w_gate", "w_up", "w_down")
SHAPES = {"w_gate": (LAYERS, D, FF), "w_up": (LAYERS, D, FF), "w_down": (LAYERS, FF, D)}


def bump(key, n, height):
    away = (jnp.arange(n, dtype=jnp.int32) - jax.random.randint(key, (), 0, n, jnp.int32)) % n
    return jnp.where(away < n // 8, height, 1.0)


def together(key, own, strength):
    shared = jax.random.normal(key, own.shape[1:], jnp.float32)
    return (own + strength * shared) * lax.rsqrt(1 + strength * strength)


def setup_inputs(seed: int = 0, part: int = 0) -> dict:
    kx, kdy, ka, kb, kz, kf, kh, kl, *kw = jax.random.split(jax.random.key(seed), 8 + len(NAMES))
    kx, kdy, ka, kb = (jax.random.fold_in(k, part) for k in (kx, kdy, ka, kb))
    shape = (SEQUENCES, TOKENS, D)
    much_x, much_dy = jax.random.uniform(kz, (2,), jnp.float32, 0.0, 1.0)
    layers = 2.0 ** jax.random.uniform(kl, (LAYERS, 1, 1), jnp.float32, -1.0, 1.0)
    x = together(ka, jax.random.normal(kx, shape, jnp.float32), much_x) * bump(kf, D, 4.0)
    dy = together(kb, jax.random.normal(kdy, shape, jnp.float32), much_dy)
    drawn = {"x": x.astype(jnp.bfloat16), "dy": (dy * (SEQUENCES * TOKENS) ** -0.5).astype(jnp.bfloat16)}
    for key, name in zip(kw, NAMES, strict=True):
        w = jax.random.normal(key, SHAPES[name], jnp.float32) * SHAPES[name][1] ** -0.5
        drawn[name] = (w * {"w_gate": 1.0, "w_up": bump(kh, FF, 4.0), "w_down": layers}[name]).astype(jnp.bfloat16)
    return drawn


def matmul(a, w):
    return jnp.dot(a, w, preferred_element_type=jnp.float32).astype(jnp.bfloat16)


def normed(h):
    wide = h.astype(jnp.float32)
    scale = lax.rsqrt(jnp.mean(wide**2, -1, keepdims=True) + 1e-6)
    return (wide * scale).astype(jnp.bfloat16)


def layer(h, w):
    a = normed(h)
    gate = jnp.dot(a, w["w_gate"], preferred_element_type=jnp.float32)
    up = jnp.dot(a, w["w_up"], preferred_element_type=jnp.float32)
    return h + matmul((jax.nn.silu(gate) * up).astype(jnp.bfloat16), w["w_down"])


def stack(weights, h):
    return lax.scan(lambda h, w: (layer(h, w), None), h, weights)[0]


def reference(x, dy, w_gate, w_up, w_down):
    weights = dict(zip(NAMES, (w_gate, w_up, w_down), strict=True))

    def take(so_far, sequence):
        h, by_y = sequence
        _, back = jax.vjp(stack, weights, h)
        by_weights, by_h = back(by_y)
        return jax.tree.map(lambda total, term: total + term.astype(jnp.float32), so_far, by_weights), by_h

    none_yet = {name: jnp.zeros(w.shape, jnp.float32) for name, w in weights.items()}
    by_weights, by_x = lax.scan(take, none_yet, (x, dy))
    return (by_x, *(by_weights[name].astype(jnp.bfloat16) for name in NAMES))
```

```python
import functools

import jax
import jax.numpy as jnp
from jax import lax
from jax.experimental import pallas as pl
from jax.experimental.pallas import tpu as pltpu
from jax.sharding import PartitionSpec as P

BF = jnp.bfloat16
F32 = jnp.float32
CHIPS = 4
TB = 512
FC = 768
VMEM_LIMIT = 66 * 2**20 - 2**21
WHERE = pl.DeviceIdType.MESH


def remote(src, dst, send, recv, to):
    return pltpu.make_async_remote_copy(
        src_ref=src, dst_ref=dst, send_sem=send, recv_sem=recv, device_id=to, device_id_type=WHERE
    )


def place():
    me, rep = lax.axis_index("dp"), lax.axis_index("rep")
    c, k = me // 2, lax.rem(me, 2)
    right = lax.rem(c + 1, CHIPS)
    left = lax.rem(c + CHIPS - 1, CHIPS)
    far = lax.rem(c + 2, CHIPS)
    return me, rep, c, k, right, left, far


def greet(devices):
    barrier = pltpu.get_barrier_semaphore()
    for d in devices:
        pl.semaphore_signal(barrier, inc=1, device_id=d, device_id_type=WHERE)
    pl.semaphore_wait(barrier, len(devices))


def normed(h):
    wide = h.astype(F32)
    scale = lax.rsqrt(jnp.mean(wide * wide, -1, keepdims=True) + 1e-6)
    return (wide * scale).astype(BF)


def dot(a, b, ca, cb):
    return lax.dot_general(a, b, (((ca,), (cb,)), ((), ())), preferred_element_type=F32)


def rows(i, n):
    return pl.ds(pl.multiple_of(i * n, n), n)


PIECES = (
    [(m, 0, j) for j in range(3) for m in ("g", "u")]
    + [("d", 0, j) for j in range(3)]
    + [("d", 1, j) for j in range(3)]
    + [(m, 1, j) for j in range(3) for m in ("g", "u")]
)
NP = len(PIECES)


def forward_kernel(
    x, dy, wg, wu, wd,
    g0, u0, hid0, a0t, h1, a1t, hid1, by1, wg_o, wu_o, wd_o,
    wgv, wuv, wdv, xv, av, atv, dyv, hv, send, recv, wsem, lsem, osem, ssem,
):
    me, rep, c, k, right, left, far = place()
    tokens, d = xv.shape
    r = lax.rem(rep, 2)
    pair = rep + 1 - 2 * r
    to_r, to_l = (rep, 2 * right + k), (rep, 2 * left + k)
    to_pair, to_core = (pair, me), (rep, me + 1 - 2 * k)
    greet([to_r, to_l, to_pair, to_core])

    full = {"g": wgv, "u": wuv, "d": wdv}
    own = {"g": wg, "u": wu, "d": wd}

    def span(u, part, own_ref=False):
        m, l, j = PIECES[u]
        third = FC // 3 if m != "d" else wdv.shape[3] // 9
        off, n = {
            "x": (r * third, 2 * third),
            "h0": (r * third, third),
            "h1": (r * third + third, third),
            "p": (2 * r * third, third),
            "all": (0, 3 * third),
        }[part]
        return pl.ds(pl.multiple_of(3 * third * j + off, third), n)

    def at(u, chip, core, part):
        m, l, j = PIECES[u]
        ref = full[m].at[l]
        s = span(u, part)
        return ref.at[chip, core, :, s] if m != "d" else ref.at[chip, core, s, :]

    def own_at(u, part):
        m, l, j = PIECES[u]
        s = span(u, part)
        return own[m].at[l, :, s] if m != "d" else own[m].at[l, s, :]

    def flow(u, f):
        s, q = send.at[u, f], recv.at[u, f]
        if f == 0:
            return remote(own_at(u, "x"), at(u, c, k, "x"), s, q, to_r)
        if f == 1:
            return remote(own_at(u, "x"), at(u, c, k, "x"), s, q, to_l)
        if f == 2:
            return remote(at(u, left, k, "h0"), at(u, left, k, "h0"), s, q, to_r)
        if f == 3:
            return remote(at(u, right, k, "h1"), at(u, right, k, "h1"), s, q, to_l)
        if f < 7:
            chip = (left, right, far)[f - 4]
            return remote(at(u, chip, k, "p"), at(u, chip, k, "p"), s, q, to_pair)
        every = pl.ds(0, CHIPS)
        return remote(at(u, every, k, "all"), at(u, every, k, "all"), s, q, to_core)

    def first(u):
        if u < NP:
            flow(u, 0).start()
            flow(u, 1).start()

    def ev1(u):
        if 0 <= u < NP:
            flow(u, 0).wait_recv()
            flow(u, 1).wait_recv()
            for f in (2, 3, 4, 5):
                flow(u, f).start()
            first(u + 2)

    def ev2(u):
        if 0 <= u < NP:
            flow(u, 2).wait_recv()
            flow(u, 3).wait_recv()
            flow(u, 6).start()

    def ev3(u):
        if 0 <= u < NP:
            for f in (4, 5, 6):
                flow(u, f).wait_recv()
            flow(u, 7).start()

    def ready(*us):
        for u in us:
            flow(u, 7).wait_recv()

    def tick(t):
        ev1(t)
        ev2(t - 1)
        ev3(t - 2)

    first(0)
    first(1)
    load_x = pltpu.make_async_copy(x, xv, lsem.at[0])
    load_dy = pltpu.make_async_copy(dy, dyv, lsem.at[1])
    load_w = [
        pltpu.make_async_copy(own[m].at[l], full[m].at[l, c, k], wsem.at[i])
        for i, (m, l) in enumerate((m, l) for m in "gud" for l in range(2))
    ]
    load_x.start()
    for w in load_w:
        w.start()
    load_dy.start()
    load_x.wait()

    def norm_block(i, _):
        a = normed(xv[rows(i, 256), :])
        av[rows(i, 256), :] = a
        atv[:, rows(i, 256)] = a.T
        return 0

    lax.fori_loop(0, tokens // 256, norm_block, 0)
    out_a0 = pltpu.make_async_copy(atv, a0t, osem.at[0])
    out_a0.start()
    for w in load_w:
        w.wait()

    nb = tokens // TB

    def columns(j):
        return slice(FC * j, FC * j + FC)

    def weight(v, l, j=None):
        w = v[l] if j is None else v[l, :, :, :, FC // 3 * j : FC // 3 * (j + 1)]
        return w.reshape(-1, w.shape[-1])

    def steps(phase_ticks, body):
        def it(i, _):
            for b, t in enumerate(phase_ticks):
                if t:
                    @pl.when(i == b)
                    def _(t=t):
                        tick(t)
            body(i)
            return 0

        lax.fori_loop(0, nb, it, 0)

    for t in range(CHIPS):
        tick(t)

    def layer0(gst, ust):
        for j in range(3):
            ready(2 * j, 2 * j + 1)

            def body(i, j=j):
                slot = lax.rem(i, 2)
                a = av[rows(i, TB), :]
                outs = [
                    pltpu.make_async_copy(st.at[slot], o.at[rows(i, TB), columns(j)], ssem.at[q, slot])
                    for q, (st, o) in enumerate(((gst, g0), (ust, u0)))
                ]
                if j > 0:
                    for o in outs:
                        o.wait()
                else:
                    @pl.when(i >= 2)
                    def _():
                        for o in outs:
                            o.wait()
                for q in range(3):
                    s, w = slice(FC // 3 * q, FC // 3 * (q + 1)), 3 * j + q
                    gate = dot(a, weight(wgv, 0, w), 1, 0)
                    up = dot(a, weight(wuv, 0, w), 1, 0)
                    gst[slot, :, s] = gate
                    ust[slot, :, s] = up
                    hv[rows(i, TB), FC // 3 * w : FC // 3 * (w + 1)] = (gate * lax.logistic(gate) * up).astype(BF)
                for o in outs:
                    o.start()

            steps(((0, 4, 0, 5), (6, 0, 7, 0), (8, 9, 0, 10))[j], body)
        for slot in range(2):
            for q, (st, o) in enumerate(((gst, g0), (ust, u0))):
                pltpu.make_async_copy(st.at[slot], o.at[rows(slot, TB), columns(0)], ssem.at[q, slot]).wait()

    stage32 = pltpu.VMEM((2, TB, FC), F32)
    pl.run_scoped(layer0, stage32, stage32)
    out_hid = pltpu.make_async_copy(hv, hid0, osem.at[1])
    out_hid.start()
    out_wg = pltpu.make_async_copy(wgv.at[0], wg_o.at[0], osem.at[2])
    out_wu = pltpu.make_async_copy(wuv.at[0], wu_o.at[0], osem.at[3])
    out_wg.start()
    out_wu.start()

    ready(6, 7, 8)
    out_a0.wait()

    def down(i):
        for q in range(2):
            part = rows(2 * i + q, TB // 2)
            out = dot(hv[part, :], weight(wdv, 0), 1, 0).astype(BF)
            h = (xv[part, :].astype(F32) + out.astype(F32)).astype(BF)
            xv[part, :] = h
            a = normed(h)
            av[part, :] = a
            atv[:, part] = a.T

    steps((0, 11, 12, 13), down)
    out_h1 = pltpu.make_async_copy(xv, h1, osem.at[4])
    out_a1 = pltpu.make_async_copy(atv, a1t, osem.at[5])
    out_wd = pltpu.make_async_copy(wdv.at[0], wd_o, osem.at[6])
    out_h1.start()
    out_a1.start()
    out_wd.start()
    out_hid.wait()
    load_dy.wait()

    ready(9, 10, 11)

    def back_down(i):
        hv[rows(i, TB), :] = dot(dyv[rows(i, TB), :], weight(wdv, 1), 1, 1).astype(BF)

    steps((0, 14, 15, 16), back_down)

    out_wg1 = pltpu.make_async_copy(wgv.at[1], wg_o.at[1], osem.at[7])
    out_wu1 = pltpu.make_async_copy(wuv.at[1], wu_o.at[1], osem.at[8])

    def layer1(st):
        outs_to = (hid1, by1.at[0], by1.at[1])

        def copies(i, j, slot):
            return [
                pltpu.make_async_copy(st.at[q, slot], o.at[rows(i, TB), columns(j)], ssem.at[q, slot])
                for q, o in enumerate(outs_to)
            ]

        for j in range(3):
            ready(12 + 2 * j, 13 + 2 * j)
            if j == 2:
                out_wg1.start()
                out_wu1.start()

            def body(i, j=j):
                slot = lax.rem(i, 2)
                a = av[rows(i, TB), :]
                outs = copies(i, j, slot)
                if j > 0:
                    for o in outs:
                        o.wait()
                else:
                    @pl.when(i >= 2)
                    def _():
                        for o in outs:
                            o.wait()
                for q in range(3):
                    s, w = slice(FC // 3 * q, FC // 3 * (q + 1)), 3 * j + q
                    gate = dot(a, weight(wgv, 1, w), 1, 0)
                    up = dot(a, weight(wuv, 1, w), 1, 0)
                    by_hid = hv[rows(i, TB), FC // 3 * w : FC // 3 * (w + 1)].astype(F32)
                    st[0, slot, :, s], st[1, slot, :, s], st[2, slot, :, s] = gated(gate, up, by_hid)
                for o in outs:
                    o.start()

            steps((0, NP - 1, NP, NP + 1) if j == 0 else (), body)
        for slot in range(2):
            for o in copies(slot, 0, slot):
                o.wait()

    pl.run_scoped(layer1, pltpu.VMEM((3, 2, TB, FC), BF))
    for o in (out_wg, out_wu, out_h1, out_a1, out_wd, out_wg1, out_wu1):
        o.wait()
    for u in range(NP):
        for f in range(8):
            flow(u, f).wait_send()


def gated(gate, up, by_hid):
    sig = lax.logistic(gate)
    silu = gate * sig
    by_silu = by_hid * up
    return (
        (silu * up).astype(BF),
        (by_silu * (sig * (1.0 + gate * (1.0 - sig)))).astype(BF),
        (by_hid * silu).astype(BF),
    )


def forward(x, dy, wg, wu, wd):
    tokens, d = x.shape
    layers, _, ff = wg.shape
    s = jax.ShapeDtypeStruct
    act, hid = s((tokens, d), BF), s((tokens, ff), BF)
    pre = s((tokens, ff), F32)
    wide = s((layers, CHIPS, 2, wg.shape[1], ff), BF)
    anyw = pl.BlockSpec(memory_space=pltpu.HBM)
    dma = pltpu.SemaphoreType.DMA
    return pl.pallas_call(
        forward_kernel,
        out_shape=(pre, pre, hid, s((d, tokens), BF), act, s((d, tokens), BF), hid, s((2, tokens, ff), BF), wide, wide, s((CHIPS, 2, wd.shape[1], d), BF)),
        in_specs=[anyw] * 5,
        out_specs=[anyw] * 11,
        scratch_shapes=[
            pltpu.VMEM(wide.shape, BF),
            pltpu.VMEM(wide.shape, BF),
            pltpu.VMEM((layers, CHIPS, 2, wd.shape[1], d), BF),
            pltpu.VMEM((tokens, d), BF),
            pltpu.VMEM((tokens, d), BF),
            pltpu.VMEM((d, tokens), BF),
            pltpu.VMEM((tokens, d), BF),
            pltpu.VMEM((tokens, ff), BF),
            dma((NP, 8)),
            dma((NP, 8)),
            dma((6,)),
            dma((2,)),
            dma((9,)),
            dma((3, 2)),
        ],
        compiler_params=pltpu.CompilerParams(collective_id=0, has_side_effects=True, vmem_limit_bytes=VMEM_LIMIT),
        name="forward",
    )(x, dy, wg, wu, wd)


NB = 256


def add(*refs):
    total = refs[0][...].astype(F32)
    for r in refs[1:]:
        total = total + r[...].astype(F32)
    return total.astype(BF)


def backward_kernel(
    dy, x, h1, a0t, a1t, hid0, hid1, by1, g0, u0, wg, wu, wd,
    dx, dwg, dwu, dwd, by0,
    td, tg, prd, rld, rrd, fld, frd, prg, rlg, rrg, flg, frg, wgv, wuv, wdv, hv, at, chunk, blk, hblk, gb, ub,
    dsend, drecv, gsend, grecv, credit, dout, gout, wsem, lsem, csem, bsem, hsem, psem, osem,
):
    me, rep, c, k, right, left, far = place()
    tokens, d = hv.shape
    to_r, to_l, to_core = (rep, 2 * right + k), (rep, 2 * left + k), (rep, me + 1 - 2 * k)
    dr = dwd.shape[1]
    once = 6 * FC // (2 * FC)

    def halves(kind, ref):
        if kind == "d":
            return ref.at[pl.ds(0, dr // 2), :], ref.at[pl.ds(dr // 2, dr // 2), :]
        return ref.at[:, pl.ds(0, FC // 2)], ref.at[:, pl.ds(FC // 2, FC // 2)]

    def mine(kind, u, chip):
        if kind == "d":
            return td.at[pl.ds(pl.multiple_of((2 * chip + k) * dr, 16), dr), :]
        return tg.at[lax.rem(u, 6), chip, k]

    def theirs(kind, u, chip):
        return prd.at[chip] if kind == "d" else prg.at[lax.rem(u, 6), chip]

    def landed(kind, u):
        if kind == "d":
            return rld, rrd, fld, frd
        return tuple(q.at[lax.rem(u, 6)] for q in (rlg, rrg, flg, frg))

    def sem(kind, u, f):
        s, q = (dsend, drecv) if kind == "d" else (gsend, grecv)
        return s.at[u, f], q.at[u, f]

    def swap(kind, u):
        if kind == "d":
            return [
                remote(td.at[pl.ds(pl.multiple_of((2 * i + 1 - k) * dr, 16), dr), :], prd.at[i], *sem(kind, u, 6 + i), to_core)
                for i in range(CHIPS)
            ]
        return [remote(tg.at[lax.rem(u, 6), :, 1 - k], prg.at[lax.rem(u, 6)], *sem(kind, u, 6), to_core)]

    def ring(kind, u, f):
        rl, rr, fl, fr = landed(kind, u)
        chip, half, to = ((far, 0, to_r), (far, 1, to_l), (right, 1, to_r), (left, 0, to_l), (right, 0, to_r), (left, 1, to_l))[f]
        land = (rl, rr)[f] if f < 2 else halves(kind, (fl, fr)[f % 2])[half]
        return remote(halves(kind, mine(kind, u, chip))[half], land, *sem(kind, u, f), to)

    def pay(kind, order, i):
        if order:
            pl.semaphore_wait(credit.at[6 if kind == "d" else i], 3)

    def begin(kind, u):
        for o in swap(kind, u):
            o.start()

    def stage1(kind, u):
        for o in swap(kind, u):
            o.wait_recv()
        f = mine(kind, u, far)
        f[...] = add(f, theirs(kind, u, far))
        ring(kind, u, 0).start()
        ring(kind, u, 1).start()
        r1, pr1 = (halves(kind, q(kind, u, right))[1] for q in (mine, theirs))
        r1[...] = add(r1, pr1)
        ring(kind, u, 2).start()
        l0, pl0 = (halves(kind, q(kind, u, left))[0] for q in (mine, theirs))
        l0[...] = add(l0, pl0)
        ring(kind, u, 3).start()

    def stage2(kind, u):
        ring(kind, u, 0).wait_recv()
        rl, rr = landed(kind, u)[:2]
        r0, pr0 = (halves(kind, q(kind, u, right))[0] for q in (mine, theirs))
        r0[...] = add(r0, pr0, rl)
        ring(kind, u, 4).start()
        ring(kind, u, 1).wait_recv()
        l1, pl1 = (halves(kind, q(kind, u, left))[1] for q in (mine, theirs))
        l1[...] = add(l1, pl1, rr)
        ring(kind, u, 5).start()

    def result(kind, u, m=0):
        src = mine(kind, u, c)
        if kind == "d":
            return pltpu.make_async_copy(src, dwd.at[1 - u], dout.at[u])
        j = lax.rem(u, 6) // 2
        to = (dwg, dwu)[m].at[1 - u // 6, :, pl.ds(pl.multiple_of(j * FC, FC), FC)]
        return pltpu.make_async_copy(src, to, gout.at[u])

    def stage3(kind, u):
        for f in (2, 3, 4, 5):
            ring(kind, u, f).wait_recv()
        m = mine(kind, u, c)
        fl, fr = landed(kind, u)[2:]
        m[...] = add(m, theirs(kind, u, c), fl, fr)
        if kind == "d":
            result(kind, u).start()
        else:
            result(kind, u, u % 2).start()
        if u < (1 if kind == "d" else 6):
            for to in (to_r, to_l, to_core):
                pl.semaphore_signal(credit.at[6 if kind == "d" else u], inc=1, device_id=to, device_id_type=WHERE)

    def end(kind, u):
        for o in swap(kind, u) + [ring(kind, u, f) for f in range(6)]:
            o.wait_send()
        result(kind, u).wait()

    def run(todo):
        for word in todo.split():
            (stage1, stage2, stage3)[int(word[0]) - 1](word[1], int(word[2], 12))

    def events(i, table):
        for b, todo in enumerate(table):
            if todo:
                @pl.when(i == b)
                def _(todo=todo):
                    run(todo)

    def piece(j):
        return pl.ds(pl.multiple_of(j * FC, FC), FC)

    def bring(src, slot):
        return pltpu.make_async_copy(src, chunk.at[slot], csem.at[slot])

    def stream(n, base, source, body, then=None):
        def it(i, _):
            slot = lax.rem(i + base, 2)

            @pl.when(i + 1 < n)
            def _():
                bring(source(i + 1), 1 - slot).start()
            if then is not None:
                @pl.when(i + 1 == n)
                def _():
                    bring(then, 1 - slot).start()
            bring(source(i), slot).wait()
            body(i, slot)
            return 0

        lax.fori_loop(0, n, it, 0)

    def grad_down(order, hid, base, table, then):
        def body(i, slot):
            events(i, table)
            for q in range(2):
                part = dot(chunk[slot, :, FC // 2 * q : FC // 2 * (q + 1)], hv[...], 0, 0).astype(BF)
                td[pl.ds(pl.multiple_of(i * FC + FC // 2 * q, FC // 2), FC // 2), :] = part

        stream(once, base, lambda i: hid.at[:, piece(i)], body, then)
        pay("d", order, 0)
        begin("d", order)

    def grad_unit(order, i, slot):
        u = 6 * order + i
        if order:
            end("g", i)
        for q in range(3):
            part = dot(at[...], chunk[slot, :, FC // 3 * q : FC // 3 * (q + 1)], 1, 0).astype(BF)
            tg[i, :, :, :, FC // 3 * q : FC // 3 * (q + 1)] = part.reshape(*tg.shape[1:4], FC // 3)
        pay("g", order, i)
        begin("g", u)

    def block_in(by, h, i, slot):
        return [
            pltpu.make_async_copy(by.at[:, rows(i, NB), :], blk.at[slot], bsem.at[slot]),
            pltpu.make_async_copy(h.at[rows(i, NB), :], hblk.at[slot], hsem.at[slot]),
        ]

    def back_norm(by, h, table):
        n = tokens // NB

        def it(i, _):
            slot = lax.rem(i, 2)

            @pl.when(i + 1 < n)
            def _():
                for o in block_in(by, h, i + 1, 1 - slot):
                    o.start()

            for o in block_in(by, h, i, slot):
                o.wait()
            events(i, table)
            by_a = dot(blk[slot, 0], wgv[...], 1, 1).astype(BF).astype(F32)
            by_a = (by_a + dot(blk[slot, 1], wuv[...], 1, 1).astype(BF).astype(F32)).astype(BF).astype(F32)
            wide = hblk[slot].astype(F32)
            s = lax.rsqrt(jnp.mean(wide * wide, -1, keepdims=True) + 1e-6)
            along = jnp.sum(by_a * wide, -1, keepdims=True) * (s * s * s * (1.0 / d))
            by_h = (by_a * s - wide * along).astype(BF).astype(F32)
            hv[rows(i, NB), :] = (hv[rows(i, NB), :].astype(F32) + by_h).astype(BF)
            return 0

        lax.fori_loop(0, n, it, 0)

    nb = tokens // TB

    def pre_in(j, b, slot):
        return [
            pltpu.make_async_copy(g0.at[rows(b, TB), piece(j)], gb.at[slot], psem.at[0, slot]),
            pltpu.make_async_copy(u0.at[rows(b, TB), piece(j)], ub.at[slot], psem.at[1, slot]),
        ]

    def by_out(q, j):
        return pltpu.make_async_copy(chunk.at[q], by0.at[q, :, piece(j)], osem.at[q])

    def back_down(j, table):
        def it(b, _):
            slot = lax.rem(b, 2)

            @pl.when(b + 1 < nb)
            def _():
                for o in pre_in(j, b + 1, 1 - slot):
                    o.start()
            if j + 1 < once:
                @pl.when(b + 1 == nb)
                def _():
                    for o in pre_in(j + 1, 0, 1 - slot):
                        o.start()
            for o in pre_in(j, b, slot):
                o.wait()
            events(b, table)
            for q in range(3):
                s = slice(FC // 3 * q, FC // 3 * (q + 1))
                w = wdv[FC * j + FC // 3 * q : FC * j + FC // 3 * (q + 1), :]
                by_hid = dot(hv[rows(b, TB), :], w, 1, 1).astype(BF).astype(F32)
                _, by_gate, by_up = gated(gb[slot, :, s], ub[slot, :, s], by_hid)
                chunk[0, rows(b, TB), s] = by_gate
                chunk[1, rows(b, TB), s] = by_up
            return 0

        lax.fori_loop(0, nb, it, 0)
        for q in range(2):
            by_out(q, j).start()

    def load_weights(l):
        return [pltpu.make_async_copy(w.at[l], v, wsem.at[i, l]) for i, (w, v) in enumerate(((wg, wgv), (wu, wuv)))]

    load_dy = pltpu.make_async_copy(dy, hv, lsem.at[0])
    load_a1 = pltpu.make_async_copy(a1t, at, lsem.at[1])
    load_a0 = pltpu.make_async_copy(a0t, at, lsem.at[2])
    load_wd = pltpu.make_async_copy(wd, wdv, wsem.at[2, 0])
    load_dy.start()
    bring(hid1.at[:, piece(0)], 0).start()
    load_a1.start()
    greet([to_r, to_l, to_core])
    load_dy.wait()

    grad_down(0, hid1, 0, (), by1.at[0, :, piece(0)])
    load_a1.wait()
    for o in load_weights(1) + [load_wd] + block_in(by1, h1, 0, 0):
        o.start()

    def last_layer(i, slot):
        grad_unit(0, i, slot)

        @pl.when(i == 1)
        def _():
            stage1("d", 0)

        @pl.when(i >= 1)
        def _():
            stage1("g", i - 1)

    stream(6, 1, lambda i: by1.at[lax.rem(i, 2), :, piece(i // 2)], last_layer, hid0.at[:, piece(0)])
    load_a0.start()
    for o in pre_in(0, 0, 0):
        o.start()
    for o in load_weights(1):
        o.wait()
    back_norm(by1, h1, ("2d0", "1g5", "2g0", "2g1", "2g2", "2g3", "", "2g4"))
    for o in load_weights(0):
        o.start()

    stage3("d", 0)
    end("d", 0)
    grad_down(1, hid0, 1, ("", "", "2g5"), None)
    load_wd.wait()
    load_a0.wait()
    tables = (("", "3g0", "3g1", "3g2"), (), ())
    after = ("1d1 3g3", "1g6 3g4 3g5", "1g7 2d1", "1g8", "1g9 2g6", "1ga 2g7")
    for j in range(once):
        if j:
            for q in range(2):
                by_out(q, j - 1).wait()
        back_down(j, tables[j])
        for q in range(2):
            grad_unit(1, 2 * j + q, q)
            run(after[2 * j + q])
            if j + 1 == once and q == 0:
                for m in range(2):
                    by_out(m, j).wait()
                for o in block_in(by0, x, 0, 0):
                    o.start()
    for o in load_weights(0):
        o.wait()
    back_norm(by0, x, ("", "1gb 2g8", "3d1", "2g9", "2ga 3g6", "", "2gb 3g7", "3g8"))
    out_dx = pltpu.make_async_copy(hv, dx, osem.at[0])
    out_dx.start()
    run("3g9 3ga 3gb")
    end("d", 1)
    for u in range(6, 12):
        end("g", u)
    out_dx.wait()


def backward(dy, x, h1, a0t, a1t, hid0, hid1, by1, g0, u0, wg, wu, wd, gate_rows, down_rows):
    tokens, d = dy.shape
    ff = g0.shape[1]
    layers = wg.shape[0]
    s = jax.ShapeDtypeStruct
    anyw = pl.BlockSpec(memory_space=pltpu.HBM)
    dma = pltpu.SemaphoreType.DMA
    v = lambda *shape: pltpu.VMEM(shape, BF)
    dr, gr, n = down_rows, gate_rows, 6 * layers
    grad = s((layers, gr, ff), BF)
    return pl.pallas_call(
        backward_kernel,
        out_shape=(s((tokens, d), BF), grad, grad, s((layers, dr, d), BF), s((2, tokens, ff), BF)),
        in_specs=[anyw] * 13,
        out_specs=[anyw] * 5,
        scratch_shapes=[
            v(ff, d),
            v(6, CHIPS, 2, gr, FC),
            v(CHIPS, dr, d),
            v(dr // 2, d),
            v(dr // 2, d),
            v(dr, d),
            v(dr, d),
            v(6, CHIPS, gr, FC),
            v(6, gr, FC // 2),
            v(6, gr, FC // 2),
            v(6, gr, FC),
            v(6, gr, FC),
            v(d, ff),
            v(d, ff),
            v(ff, d),
            v(tokens, d),
            v(d, tokens),
            v(2, tokens, FC),
            v(2, 2, NB, ff),
            v(2, NB, d),
            pltpu.VMEM((2, TB, FC), F32),
            pltpu.VMEM((2, TB, FC), F32),
            dma((layers, 10)),
            dma((layers, 10)),
            dma((n, 7)),
            dma((n, 7)),
            pltpu.SemaphoreType.REGULAR((7,)),
            dma((layers,)),
            dma((n,)),
            dma((3, layers)),
            dma((3,)),
            dma((2,)),
            dma((2,)),
            dma((2,)),
            dma((2, 2)),
            dma((2,)),
        ],
        compiler_params=pltpu.CompilerParams(collective_id=1, has_side_effects=True, vmem_limit_bytes=VMEM_LIMIT),
        name="backward",
    )(dy, x, h1, a0t, a1t, hid0, hid1, by1, g0, u0, wg, wu, wd)


def solution(mesh):
    assert mesh.shape["dp"] == 2 * CHIPS and mesh.shape["rep"] % 2 == 0

    def step(x, dy, wg, wu, wd):
        x, dy = x[0], dy[0]
        layers, gr, ff = wg.shape
        dr, d = wd.shape[1:]
        g0, u0, hid0, a0t, h1, a1t, hid1, by1, wg_all, wu_all, wd_all = forward(x, dy, wg, wu, wd)
        wg_all, wu_all = (w.reshape(layers, d, ff) for w in (wg_all, wu_all))
        dx, dwg, dwu, dwd, _ = backward(
            dy, x, h1, a0t, a1t, hid0, hid1, by1, g0, u0, wg_all, wu_all, wd_all.reshape(ff, d), gr, dr
        )
        return dx[None], dwg, dwu, dwd

    tokens, weight = P(("rep", "dp")), P(None, "dp")
    grad = P("rep", "dp")
    return jax.shard_map(
        step,
        mesh=mesh,
        in_specs=(tokens, tokens, weight, weight, weight),
        out_specs=(tokens, grad, grad, grad),
        check_vma=False,
    )
```

```python
import functools

import jax
import jax.numpy as jnp
from jax import lax
from jax.experimental import pallas as pl
from jax.experimental.pallas import tpu as pltpu
from jax.sharding import PartitionSpec as P

BF = jnp.bfloat16
F32 = jnp.float32
CHIPS = 4
TB = 512
FC = 768
VMEM_LIMIT = 66 * 2**20 - 2**21
WHERE = pl.DeviceIdType.MESH


def remote(src, dst, send, recv, to):
    return pltpu.make_async_remote_copy(
        src_ref=src, dst_ref=dst, send_sem=send, recv_sem=recv, device_id=to, device_id_type=WHERE
    )


def place():
    me, rep = lax.axis_index("dp"), lax.axis_index("rep")
    c, k = me // 2, lax.rem(me, 2)
    right = lax.rem(c + 1, CHIPS)
    left = lax.rem(c + CHIPS - 1, CHIPS)
    far = lax.rem(c + 2, CHIPS)
    return me, rep, c, k, right, left, far


def greet(devices):
    barrier = pltpu.get_barrier_semaphore()
    for d in devices:
        pl.semaphore_signal(barrier, inc=1, device_id=d, device_id_type=WHERE)
    pl.semaphore_wait(barrier, len(devices))


def normed(h):
    wide = h.astype(F32)
    scale = lax.rsqrt(jnp.mean(wide * wide, -1, keepdims=True) + 1e-6)
    return (wide * scale).astype(BF)


def dot(a, b, ca, cb):
    return lax.dot_general(a, b, (((ca,), (cb,)), ((), ())), preferred_element_type=F32)


def rows(i, n):
    return pl.ds(pl.multiple_of(i * n, n), n)


PIECES = (
    [(m, 0, j) for j in range(3) for m in ("g", "u")]
    + [("d", 0, j) for j in range(3)]
    + [("d", 1, j) for j in range(3)]
    + [(m, 1, j) for j in range(3) for m in ("g", "u")]
)
NP = len(PIECES)


def forward_kernel(
    x, dy, wg, wu, wd,
    g0, u0, hid0, a0t, h1, a1t, hid1, by1, wg_o, wu_o, wd_o,
    wgv, wuv, wdv, xv, av, atv, dyv, hv, send, recv, wsem, lsem, osem, ssem,
):
    me, rep, c, k, right, left, far = place()
    tokens, d = xv.shape
    r = lax.rem(rep, 2)
    pair = rep + 1 - 2 * r
    to_r, to_l = (rep, 2 * right + k), (rep, 2 * left + k)
    to_pair, to_core = (pair, me), (rep, me + 1 - 2 * k)
    greet([to_r, to_l, to_pair, to_core])

    full = {"g": wgv, "u": wuv, "d": wdv}
    own = {"g": wg, "u": wu, "d": wd}

    def span(u, part, own_ref=False):
        m, l, j = PIECES[u]
        third = FC // 3 if m != "d" else wdv.shape[3] // 9
        off, n = {
            "x": (r * third, 2 * third),
            "h0": (r * third, third),
            "h1": (r * third + third, third),
            "p": (2 * r * third, third),
            "all": (0, 3 * third),
        }[part]
        return pl.ds(pl.multiple_of(3 * third * j + off, third), n)

    def at(u, chip, core, part):
        m, l, j = PIECES[u]
        ref = full[m].at[l]
        s = span(u, part)
        return ref.at[chip, core, :, s] if m != "d" else ref.at[chip, core, s, :]

    def own_at(u, part):
        m, l, j = PIECES[u]
        s = span(u, part)
        return own[m].at[l, :, s] if m != "d" else own[m].at[l, s, :]

    def flow(u, f):
        s, q = send.at[u, f], recv.at[u, f]
        if f == 0:
            return remote(own_at(u, "x"), at(u, c, k, "x"), s, q, to_r)
        if f == 1:
            return remote(own_at(u, "x"), at(u, c, k, "x"), s, q, to_l)
        if f == 2:
            return remote(at(u, left, k, "h0"), at(u, left, k, "h0"), s, q, to_r)
        if f == 3:
            return remote(at(u, right, k, "h1"), at(u, right, k, "h1"), s, q, to_l)
        if f < 7:
            chip = (left, right, far)[f - 4]
            return remote(at(u, chip, k, "p"), at(u, chip, k, "p"), s, q, to_pair)
        every = pl.ds(0, CHIPS)
        return remote(at(u, every, k, "all"), at(u, every, k, "all"), s, q, to_core)

    def first(u):
        if u < NP:
            flow(u, 0).start()
            flow(u, 1).start()

    def ev1(u):
        if 0 <= u < NP:
            flow(u, 0).wait_recv()
            flow(u, 1).wait_recv()
            for f in (2, 3, 4, 5):
                flow(u, f).start()
            first(u + 2)

    def ev2(u):
        if 0 <= u < NP:
            flow(u, 2).wait_recv()
            flow(u, 3).wait_recv()
            flow(u, 6).start()

    def ev3(u):
        if 0 <= u < NP:
            for f in (4, 5, 6):
                flow(u, f).wait_recv()
            flow(u, 7).start()

    def ready(*us):
        for u in us:
            flow(u, 7).wait_recv()

    def tick(t):
        ev1(t)
        ev2(t - 1)
        ev3(t - 2)

    first(0)
    first(1)
    load_x = pltpu.make_async_copy(x, xv, lsem.at[0])
    load_dy = pltpu.make_async_copy(dy, dyv, lsem.at[1])
    load_w = [
        pltpu.make_async_copy(own[m].at[l], full[m].at[l, c, k], wsem.at[i])
        for i, (m, l) in enumerate((m, l) for m in "gud" for l in range(2))
    ]
    load_x.start()
    for w in load_w:
        w.start()
    load_dy.start()
    load_x.wait()

    def norm_block(i, _):
        a = normed(xv[rows(i, 256), :])
        av[rows(i, 256), :] = a
        atv[:, rows(i, 256)] = a.T
        return 0

    lax.fori_loop(0, tokens // 256, norm_block, 0)
    out_a0 = pltpu.make_async_copy(atv, a0t, osem.at[0])
    out_a0.start()
    for w in load_w:
        w.wait()

    nb = tokens // TB

    def columns(j):
        return slice(FC * j, FC * j + FC)

    def weight(v, l, j=None):
        w = v[l] if j is None else v[l, :, :, :, FC // 3 * j : FC // 3 * (j + 1)]
        return w.reshape(-1, w.shape[-1])

    def steps(phase_ticks, body):
        def it(i, _):
            for b, t in enumerate(phase_ticks):
                if t:
                    @pl.when(i == b)
                    def _(t=t):
                        tick(t)
            body(i)
            return 0

        lax.fori_loop(0, nb, it, 0)

    for t in range(CHIPS):
        tick(t)

    def layer0(gst, ust):
        for j in range(3):
            ready(2 * j, 2 * j + 1)

            def body(i, j=j):
                slot = lax.rem(i, 2)
                a = av[rows(i, TB), :]
                outs = [
                    pltpu.make_async_copy(st.at[slot], o.at[rows(i, TB), columns(j)], ssem.at[q, slot])
                    for q, (st, o) in enumerate(((gst, g0), (ust, u0)))
                ]
                if j > 0:
                    for o in outs:
                        o.wait()
                else:
                    @pl.when(i >= 2)
                    def _():
                        for o in outs:
                            o.wait()
                for q in range(3):
                    s, w = slice(FC // 3 * q, FC // 3 * (q + 1)), 3 * j + q
                    gate = dot(a, weight(wgv, 0, w), 1, 0)
                    up = dot(a, weight(wuv, 0, w), 1, 0)
                    gst[slot, :, s] = gate
                    ust[slot, :, s] = up
                    hv[rows(i, TB), FC // 3 * w : FC // 3 * (w + 1)] = (gate * lax.logistic(gate) * up).astype(BF)
                for o in outs:
                    o.start()

            steps(((0, 4, 0, 5), (6, 0, 7, 0), (8, 9, 0, 10))[j], body)
        for slot in range(2):
            for q, (st, o) in enumerate(((gst, g0), (ust, u0))):
                pltpu.make_async_copy(st.at[slot], o.at[rows(slot, TB), columns(0)], ssem.at[q, slot]).wait()

    stage32 = pltpu.VMEM((2, TB, FC), F32)
    pl.run_scoped(layer0, stage32, stage32)
    out_hid = pltpu.make_async_copy(hv, hid0, osem.at[1])
    out_hid.start()
    out_wg = pltpu.make_async_copy(wgv.at[0], wg_o.at[0], osem.at[2])
    out_wu = pltpu.make_async_copy(wuv.at[0], wu_o.at[0], osem.at[3])
    out_wg.start()
    out_wu.start()

    ready(6, 7, 8)
    out_a0.wait()

    def down(i):
        for q in range(2):
            part = rows(2 * i + q, TB // 2)
            out = dot(hv[part, :], weight(wdv, 0), 1, 0).astype(BF)
            h = (xv[part, :].astype(F32) + out.astype(F32)).astype(BF)
            xv[part, :] = h
            a = normed(h)
            av[part, :] = a
            atv[:, part] = a.T

    steps((0, 11, 12, 13), down)
    out_h1 = pltpu.make_async_copy(xv, h1, osem.at[4])
    out_a1 = pltpu.make_async_copy(atv, a1t, osem.at[5])
    out_wd = pltpu.make_async_copy(wdv.at[0], wd_o, osem.at[6])
    out_h1.start()
    out_a1.start()
    out_wd.start()
    out_hid.wait()
    load_dy.wait()

    ready(9, 10, 11)

    def back_down(i):
        hv[rows(i, TB), :] = dot(dyv[rows(i, TB), :], weight(wdv, 1), 1, 1).astype(BF)

    steps((0, 14, 15, 16), back_down)

    out_wg1 = pltpu.make_async_copy(wgv.at[1], wg_o.at[1], osem.at[7])
    out_wu1 = pltpu.make_async_copy(wuv.at[1], wu_o.at[1], osem.at[8])

    def layer1(st):
        outs_to = (hid1, by1.at[0], by1.at[1])

        def copies(i, j, slot):
            return [
                pltpu.make_async_copy(st.at[q, slot], o.at[rows(i, TB), columns(j)], ssem.at[q, slot])
                for q, o in enumerate(outs_to)
            ]

        for j in range(3):
            ready(12 + 2 * j, 13 + 2 * j)
            if j == 2:
                out_wg1.start()
                out_wu1.start()

            def body(i, j=j):
                slot = lax.rem(i, 2)
                a = av[rows(i, TB), :]
                outs = copies(i, j, slot)
                if j > 0:
                    for o in outs:
                        o.wait()
                else:
                    @pl.when(i >= 2)
                    def _():
                        for o in outs:
                            o.wait()
                for q in range(3):
                    s, w = slice(FC // 3 * q, FC // 3 * (q + 1)), 3 * j + q
                    gate = dot(a, weight(wgv, 1, w), 1, 0)
                    up = dot(a, weight(wuv, 1, w), 1, 0)
                    by_hid = hv[rows(i, TB), FC // 3 * w : FC // 3 * (w + 1)].astype(F32)
                    st[0, slot, :, s], st[1, slot, :, s], st[2, slot, :, s] = gated(gate, up, by_hid)
                for o in outs:
                    o.start()

            steps((0, NP - 1, NP, NP + 1) if j == 0 else (), body)
        for slot in range(2):
            for o in copies(slot, 0, slot):
                o.wait()

    pl.run_scoped(layer1, pltpu.VMEM((3, 2, TB, FC), BF))
    for o in (out_wg, out_wu, out_h1, out_a1, out_wd, out_wg1, out_wu1):
        o.wait()
    for u in range(NP):
        for f in range(8):
            flow(u, f).wait_send()


def gated(gate, up, by_hid):
    sig = lax.logistic(gate)
    silu = gate * sig
    by_silu = by_hid * up
    return (
        (silu * up).astype(BF),
        (by_silu * (sig * (1.0 + gate * (1.0 - sig)))).astype(BF),
        (by_hid * silu).astype(BF),
    )


def forward(x, dy, wg, wu, wd):
    tokens, d = x.shape
    layers, _, ff = wg.shape
    s = jax.ShapeDtypeStruct
    act, hid = s((tokens, d), BF), s((tokens, ff), BF)
    pre = s((tokens, ff), F32)
    wide = s((layers, CHIPS, 2, wg.shape[1], ff), BF)
    anyw = pl.BlockSpec(memory_space=pltpu.HBM)
    dma = pltpu.SemaphoreType.DMA
    return pl.pallas_call(
        forward_kernel,
        out_shape=(pre, pre, hid, s((d, tokens), BF), act, s((d, tokens), BF), hid, s((2, tokens, ff), BF), wide, wide, s((CHIPS, 2, wd.shape[1], d), BF)),
        in_specs=[anyw] * 5,
        out_specs=[anyw] * 11,
        scratch_shapes=[
            pltpu.VMEM(wide.shape, BF),
            pltpu.VMEM(wide.shape, BF),
            pltpu.VMEM((layers, CHIPS, 2, wd.shape[1], d), BF),
            pltpu.VMEM((tokens, d), BF),
            pltpu.VMEM((tokens, d), BF),
            pltpu.VMEM((d, tokens), BF),
            pltpu.VMEM((tokens, d), BF),
            pltpu.VMEM((tokens, ff), BF),
            dma((NP, 8)),
            dma((NP, 8)),
            dma((6,)),
            dma((2,)),
            dma((9,)),
            dma((3, 2)),
        ],
        compiler_params=pltpu.CompilerParams(collective_id=0, has_side_effects=True, vmem_limit_bytes=VMEM_LIMIT),
        name="forward",
    )(x, dy, wg, wu, wd)


NB = 256


def add(*refs):
    total = refs[0][...].astype(F32)
    for r in refs[1:]:
        total = total + r[...].astype(F32)
    return total.astype(BF)


def backward_kernel(
    dy, x, h1, a0t, a1t, hid0, hid1, by1, g0, u0, wg, wu, wd,
    dx, dwg, dwu, dwd, by0,
    td, tg, prd, rld, rrd, fld, frd, prg, rlg, rrg, flg, frg, wgv, wuv, wdv, hv, at, chunk, blk, hblk, gb, ub,
    dsend, drecv, gsend, grecv, credit, dout, gout, wsem, lsem, csem, bsem, hsem, psem, osem,
):
    me, rep, c, k, right, left, far = place()
    tokens, d = hv.shape
    to_r, to_l, to_core = (rep, 2 * right + k), (rep, 2 * left + k), (rep, me + 1 - 2 * k)
    dr = dwd.shape[1]
    once = 6 * FC // (2 * FC)

    def halves(kind, ref):
        if kind == "d":
            return ref.at[pl.ds(0, dr // 2), :], ref.at[pl.ds(dr // 2, dr // 2), :]
        return ref.at[:, pl.ds(0, FC // 2)], ref.at[:, pl.ds(FC // 2, FC // 2)]

    def mine(kind, u, chip):
        if kind == "d":
            return td.at[pl.ds(pl.multiple_of((2 * chip + k) * dr, 16), dr), :]
        return tg.at[lax.rem(u, 6), chip, k]

    def theirs(kind, u, chip):
        return prd.at[chip] if kind == "d" else prg.at[lax.rem(u, 6), chip]

    def landed(kind, u):
        if kind == "d":
            return rld, rrd, fld, frd
        return tuple(q.at[lax.rem(u, 6)] for q in (rlg, rrg, flg, frg))

    def sem(kind, u, f):
        s, q = (dsend, drecv) if kind == "d" else (gsend, grecv)
        return s.at[u, f], q.at[u, f]

    def swap(kind, u):
        if kind == "d":
            return [
                remote(td.at[pl.ds(pl.multiple_of((2 * i + 1 - k) * dr, 16), dr), :], prd.at[i], *sem(kind, u, 6 + i), to_core)
                for i in range(CHIPS)
            ]
        return [remote(tg.at[lax.rem(u, 6), :, 1 - k], prg.at[lax.rem(u, 6)], *sem(kind, u, 6), to_core)]

    def ring(kind, u, f):
        rl, rr, fl, fr = landed(kind, u)
        chip, half, to = ((far, 0, to_r), (far, 1, to_l), (right, 1, to_r), (left, 0, to_l), (right, 0, to_r), (left, 1, to_l))[f]
        land = (rl, rr)[f] if f < 2 else halves(kind, (fl, fr)[f % 2])[half]
        return remote(halves(kind, mine(kind, u, chip))[half], land, *sem(kind, u, f), to)

    def pay(kind, order, i):
        if order:
            pl.semaphore_wait(credit.at[6 if kind == "d" else i], 3)

    def begin(kind, u):
        for o in swap(kind, u):
            o.start()

    def stage1(kind, u):
        for o in swap(kind, u):
            o.wait_recv()
        f = mine(kind, u, far)
        f[...] = add(f, theirs(kind, u, far))
        ring(kind, u, 0).start()
        ring(kind, u, 1).start()
        r1, pr1 = (halves(kind, q(kind, u, right))[1] for q in (mine, theirs))
        r1[...] = add(r1, pr1)
        ring(kind, u, 2).start()
        l0, pl0 = (halves(kind, q(kind, u, left))[0] for q in (mine, theirs))
        l0[...] = add(l0, pl0)
        ring(kind, u, 3).start()

    def stage2(kind, u):
        ring(kind, u, 0).wait_recv()
        rl, rr = landed(kind, u)[:2]
        r0, pr0 = (halves(kind, q(kind, u, right))[0] for q in (mine, theirs))
        r0[...] = add(r0, pr0, rl)
        ring(kind, u, 4).start()
        ring(kind, u, 1).wait_recv()
        l1, pl1 = (halves(kind, q(kind, u, left))[1] for q in (mine, theirs))
        l1[...] = add(l1, pl1, rr)
        ring(kind, u, 5).start()

    def result(kind, u, m=0):
        src = mine(kind, u, c)
        if kind == "d":
            return pltpu.make_async_copy(src, dwd.at[1 - u], dout.at[u])
        j = lax.rem(u, 6) // 2
        to = (dwg, dwu)[m].at[1 - u // 6, :, pl.ds(pl.multiple_of(j * FC, FC), FC)]
        return pltpu.make_async_copy(src, to, gout.at[u])

    def stage3(kind, u):
        for f in (2, 3, 4, 5):
            ring(kind, u, f).wait_recv()
        m = mine(kind, u, c)
        fl, fr = landed(kind, u)[2:]
        m[...] = add(m, theirs(kind, u, c), fl, fr)
        if kind == "d":
            result(kind, u).start()
        else:
            result(kind, u, u % 2).start()
        if u < (1 if kind == "d" else 6):
            for to in (to_r, to_l, to_core):
                pl.semaphore_signal(credit.at[6 if kind == "d" else u], inc=1, device_id=to, device_id_type=WHERE)

    def end(kind, u):
        for o in swap(kind, u) + [ring(kind, u, f) for f in range(6)]:
            o.wait_send()
        result(kind, u).wait()

    def run(todo):
        for word in todo.split():
            (stage1, stage2, stage3)[int(word[0]) - 1](word[1], int(word[2], 12))

    def events(i, table):
        for b, todo in enumerate(table):
            if todo:
                @pl.when(i == b)
                def _(todo=todo):
                    run(todo)

    def piece(j):
        return pl.ds(pl.multiple_of(j * FC, FC), FC)

    def bring(src, slot):
        return pltpu.make_async_copy(src, chunk.at[slot], csem.at[slot])

    def stream(n, base, source, body, then=None):
        def it(i, _):
            slot = lax.rem(i + base, 2)

            @pl.when(i + 1 < n)
            def _():
                bring(source(i + 1), 1 - slot).start()
            if then is not None:
                @pl.when(i + 1 == n)
                def _():
                    bring(then, 1 - slot).start()
            bring(source(i), slot).wait()
            body(i, slot)
            return 0

        lax.fori_loop(0, n, it, 0)

    def grad_down(order, hid, base, table, then):
        def body(i, slot):
            events(i, table)
            for q in range(2):
                part = dot(chunk[slot, :, FC // 2 * q : FC // 2 * (q + 1)], hv[...], 0, 0).astype(BF)
                td[pl.ds(pl.multiple_of(i * FC + FC // 2 * q, FC // 2), FC // 2), :] = part

        stream(once, base, lambda i: hid.at[:, piece(i)], body, then)
        pay("d", order, 0)
        begin("d", order)

    def grad_unit(order, i, slot):
        u = 6 * order + i
        if order:
            end("g", i)
        for q in range(3):
            part = dot(at[...], chunk[slot, :, FC // 3 * q : FC // 3 * (q + 1)], 1, 0).astype(BF)
            tg[i, :, :, :, FC // 3 * q : FC // 3 * (q + 1)] = part.reshape(*tg.shape[1:4], FC // 3)
        pay("g", order, i)
        begin("g", u)

    def block_in(by, h, i, slot):
        return [
            pltpu.make_async_copy(by.at[:, rows(i, NB), :], blk.at[slot], bsem.at[slot]),
            pltpu.make_async_copy(h.at[rows(i, NB), :], hblk.at[slot], hsem.at[slot]),
        ]

    def back_norm(by, h, table):
        n = tokens // NB

        def it(i, _):
            slot = lax.rem(i, 2)

            @pl.when(i + 1 < n)
            def _():
                for o in block_in(by, h, i + 1, 1 - slot):
                    o.start()

            for o in block_in(by, h, i, slot):
                o.wait()
            events(i, table)
            by_a = dot(blk[slot, 0], wgv[...], 1, 1).astype(BF).astype(F32)
            by_a = (by_a + dot(blk[slot, 1], wuv[...], 1, 1).astype(BF).astype(F32)).astype(BF).astype(F32)
            wide = hblk[slot].astype(F32)
            s = lax.rsqrt(jnp.mean(wide * wide, -1, keepdims=True) + 1e-6)
            along = jnp.sum(by_a * wide, -1, keepdims=True) * (s * s * s * (1.0 / d))
            by_h = (by_a * s - wide * along).astype(BF).astype(F32)
            hv[rows(i, NB), :] = (hv[rows(i, NB), :].astype(F32) + by_h).astype(BF)
            return 0

        lax.fori_loop(0, n, it, 0)

    nb = tokens // TB

    def pre_in(j, b, slot):
        return [
            pltpu.make_async_copy(g0.at[rows(b, TB), piece(j)], gb.at[slot], psem.at[0, slot]),
            pltpu.make_async_copy(u0.at[rows(b, TB), piece(j)], ub.at[slot], psem.at[1, slot]),
        ]

    def by_out(q, j):
        return pltpu.make_async_copy(chunk.at[q], by0.at[q, :, piece(j)], osem.at[q])

    def back_down(j, table):
        def it(b, _):
            slot = lax.rem(b, 2)

            @pl.when(b + 1 < nb)
            def _():
                for o in pre_in(j, b + 1, 1 - slot):
                    o.start()

            @pl.when((b + 1 == nb) & (j + 1 < once))
            def _():
                for o in pre_in(j + 1, 0, 1 - slot):
                    o.start()

            for o in pre_in(j, b, slot):
                o.wait()
            events(b + nb * j, table)
            for q in range(3):
                s = slice(FC // 3 * q, FC // 3 * (q + 1))
                w = wdv[rows(3 * j + q, FC // 3), :]
                by_hid = dot(hv[rows(b, TB), :], w, 1, 1).astype(BF).astype(F32)
                _, by_gate, by_up = gated(gb[slot, :, s], ub[slot, :, s], by_hid)
                chunk[0, rows(b, TB), s] = by_gate
                chunk[1, rows(b, TB), s] = by_up
            return 0

        lax.fori_loop(0, nb, it, 0)
        for q in range(2):
            by_out(q, j).start()

    def load_weights(l):
        return [pltpu.make_async_copy(w.at[l], v, wsem.at[i, l]) for i, (w, v) in enumerate(((wg, wgv), (wu, wuv)))]

    load_dy = pltpu.make_async_copy(dy, hv, lsem.at[0])
    load_a1 = pltpu.make_async_copy(a1t, at, lsem.at[1])
    load_a0 = pltpu.make_async_copy(a0t, at, lsem.at[2])
    load_wd = pltpu.make_async_copy(wd, wdv, wsem.at[2, 0])
    load_dy.start()
    bring(hid1.at[:, piece(0)], 0).start()
    load_a1.start()
    greet([to_r, to_l, to_core])
    load_dy.wait()

    grad_down(0, hid1, 0, (), by1.at[0, :, piece(0)])
    load_a1.wait()
    for o in load_weights(1) + [load_wd] + block_in(by1, h1, 0, 0):
        o.start()

    def last_layer(i, slot):
        grad_unit(0, i, slot)

        @pl.when(i == 1)
        def _():
            stage1("d", 0)

        @pl.when(i >= 1)
        def _():
            stage1("g", i - 1)

    stream(6, 1, lambda i: by1.at[lax.rem(i, 2), :, piece(i // 2)], last_layer, hid0.at[:, piece(0)])
    load_a0.start()
    for o in pre_in(0, 0, 0):
        o.start()
    for o in load_weights(1):
        o.wait()
    back_norm(by1, h1, ("2d0", "1g5", "2g0", "2g1", "2g2", "2g3", "", "2g4"))
    for o in load_weights(0):
        o.start()

    stage3("d", 0)
    end("d", 0)
    grad_down(1, hid0, 1, ("", "", "2g5"), None)
    load_wd.wait()
    load_a0.wait()
    after = ("1d1 3g3", "1g6 3g4 3g5", "1g7 2d1", "1g8", "1g9 2g6", "1ga 2g7")

    def first_layer(j, _):
        @pl.when(j > 0)
        def _():
            for q in range(2):
                by_out(q, j - 1).wait()

        back_down(j, ("", "3g0", "3g1", "3g2"))
        for q in range(2):
            grad_unit(1, 2 * j + q, q)
            events(2 * j + q, after)
            if q == 0:
                @pl.when(j + 1 == once)
                def _():
                    for m in range(2):
                        by_out(m, j).wait()
                    for o in block_in(by0, x, 0, 0):
                        o.start()
        return 0

    lax.fori_loop(0, once, first_layer, 0)
    for o in load_weights(0):
        o.wait()
    back_norm(by0, x, ("", "1gb 2g8", "3d1", "2g9", "2ga 3g6", "", "2gb 3g7", "3g8"))
    out_dx = pltpu.make_async_copy(hv, dx, osem.at[0])
    out_dx.start()
    run("3g9 3ga 3gb")
    end("d", 1)
    for u in range(6, 12):
        end("g", u)
    out_dx.wait()


def backward(dy, x, h1, a0t, a1t, hid0, hid1, by1, g0, u0, wg, wu, wd, gate_rows, down_rows):
    tokens, d = dy.shape
    ff = g0.shape[1]
    layers = wg.shape[0]
    s = jax.ShapeDtypeStruct
    anyw = pl.BlockSpec(memory_space=pltpu.HBM)
    dma = pltpu.SemaphoreType.DMA
    v = lambda *shape: pltpu.VMEM(shape, BF)
    dr, gr, n = down_rows, gate_rows, 6 * layers
    grad = s((layers, gr, ff), BF)
    return pl.pallas_call(
        backward_kernel,
        out_shape=(s((tokens, d), BF), grad, grad, s((layers, dr, d), BF), s((2, tokens, ff), BF)),
        in_specs=[anyw] * 13,
        out_specs=[anyw] * 5,
        scratch_shapes=[
            v(ff, d),
            v(6, CHIPS, 2, gr, FC),
            v(CHIPS, dr, d),
            v(dr // 2, d),
            v(dr // 2, d),
            v(dr, d),
            v(dr, d),
            v(6, CHIPS, gr, FC),
            v(6, gr, FC // 2),
            v(6, gr, FC // 2),
            v(6, gr, FC),
            v(6, gr, FC),
            v(d, ff),
            v(d, ff),
            v(ff, d),
            v(tokens, d),
            v(d, tokens),
            v(2, tokens, FC),
            v(2, 2, NB, ff),
            v(2, NB, d),
            pltpu.VMEM((2, TB, FC), F32),
            pltpu.VMEM((2, TB, FC), F32),
            dma((layers, 10)),
            dma((layers, 10)),
            dma((n, 7)),
            dma((n, 7)),
            pltpu.SemaphoreType.REGULAR((7,)),
            dma((layers,)),
            dma((n,)),
            dma((3, layers)),
            dma((3,)),
            dma((2,)),
            dma((2,)),
            dma((2,)),
            dma((2, 2)),
            dma((2,)),
        ],
        compiler_params=pltpu.CompilerParams(collective_id=1, has_side_effects=True, vmem_limit_bytes=VMEM_LIMIT),
        name="backward",
    )(dy, x, h1, a0t, a1t, hid0, hid1, by1, g0, u0, wg, wu, wd)


def solution(mesh):
    assert mesh.shape["dp"] == 2 * CHIPS and mesh.shape["rep"] % 2 == 0

    def step(x, dy, wg, wu, wd):
        x, dy = x[0], dy[0]
        layers, gr, ff = wg.shape
        dr, d = wd.shape[1:]
        g0, u0, hid0, a0t, h1, a1t, hid1, by1, wg_all, wu_all, wd_all = forward(x, dy, wg, wu, wd)
        wg_all, wu_all = (w.reshape(layers, d, ff) for w in (wg_all, wu_all))
        dx, dwg, dwu, dwd, _ = backward(
            dy, x, h1, a0t, a1t, hid0, hid1, by1, g0, u0, wg_all, wu_all, wd_all.reshape(ff, d), gr, dr
        )
        return dx[None], dwg, dwu, dwd

    tokens, weight = P(("rep", "dp")), P(None, "dp")
    grad = P("rep", "dp")
    return jax.shard_map(
        step,
        mesh=mesh,
        in_specs=(tokens, tokens, weight, weight, weight),
        out_specs=(tokens, grad, grad, grad),
        check_vma=False,
    )
```
